512 devices in a mesh: grp: 16 (over y, z_hi, core), dev: 32 (over z_lo, x).
Axes of the slice: x: 4, y: 4, z: 16 (z_hi: 2, z_lo: 8; z = z_hi * 8 + z_lo), core: 2. Of those that a mesh axis runs over, the one named last changes fastest.
Arguments:
- train_grads: bfloat16 [65536, 1024], P(('grp', 'dev')), may hold values from -192 to 192, as said below
- queries: bfloat16 [2048, 1024], P('grp'), may hold values from -6 to 6
Outputs:
- scores: bfloat16 [65536, 2048], P(('grp', 'dev'))
The draws below stay inside these ranges and needn't reach their ends.
Inputs may be any that keep to these rules, and one draw needn't show every extreme that they name: `train_grads`: Real-valued projected gradients whose columns and rows differ in scale.
All inputs are finite; a program needn't handle non-finite values. Where the reference program divides by a largest or mean magnitude, that divisor is 1e-20 or more.
Results may differ from the reference program's by a relative error of at most 0.001.
The reference program's roundings to bfloat16 on the way (of `prepared`) count: a program that leaves them out, or rounds other values in their place, can miss the bound.
Values may be sent and summed in bfloat16 or wider, within the bound.
A program may use at most 64 MiB of HBM per device.

```python
import jax
import jax.numpy as jnp
from jax import lax

K = 1024
ROWS_DEV = 128
ITERS = 8
TOTAL = 65536
QTOT = 2048
N_GRP = 16
N_DEV = 32


def draw_train_grads(key, part):
    key_cols = jax.random.fold_in(key, 11)
    key_perm = jax.random.fold_in(key, 12)
    key_base = jax.random.fold_in(key, 13)
    colscale = jnp.exp(jax.random.uniform(key_cols, (K,), jnp.float32, 0.0, jnp.log(10.0)))
    order = jax.random.permutation(key_perm, K)
    position = jnp.arange(TOTAL, dtype=jnp.float32) / TOTAL
    rowscale = jnp.exp(jnp.log(3.0) * position)
    base = jnp.clip(jax.random.normal(key_base, (TOTAL, K), jnp.float32), -4.0, 4.0)
    mixed = base + 0.6 * base[:, order]
    return (mixed * colscale[None, :] * rowscale[:, None]).astype(jnp.bfloat16)


def block_levels(own_key, shape, pieces, low, top_value):
    def one(dim, blocks):
        draws = jax.random.uniform(jax.random.fold_in(jax.random.fold_in(own_key, 6), dim), (blocks,), jnp.float32, low / len(pieces), top_value / len(pieces))
        return jnp.repeat(jnp.exp(draws), shape[dim] // blocks).reshape((-1,) + (1,) * (len(shape) - dim - 1))

    gain = one(*pieces[0])
    for cut in pieces[1:]:
        gain = gain * one(*cut)
    return gain


def centred(rng, extent, width, most, pieces=(), held_as=jnp.bfloat16):
    loudness = block_levels(rng, extent, pieces, -0.22, 0.18) if pieces else 1.0
    drawn = jax.random.normal(rng, extent, jnp.float32) * width * loudness
    return jnp.minimum(jnp.maximum(drawn, -most), most).astype(held_as)


def setup_inputs(seed: int = 0) -> dict:
    arg_keys = jax.random.split(jax.random.key(seed), 3)
    return {
        "train_grads": draw_train_grads(jax.random.fold_in(arg_keys[2], 71), 0),
        "queries": centred(arg_keys[1], (QTOT, K), 1.0, 6.0, ((0, 16),)),
    }


damping_ratio = 0.1


def reference(train_grads, queries):
    gram = lax.dot_general(train_grads, train_grads, (((0,), (0,)), ((), ())), preferred_element_type=jnp.float32)
    normed = gram / TOTAL
    mean_eig = jnp.trace(gram) / (TOTAL * K)
    damp = damping_ratio * mean_eig
    bound = jnp.max(jnp.sum(jnp.abs(normed), axis=1)) + damp
    step = 1.0 / bound
    oper = normed + damp * jnp.eye(K, dtype=jnp.float32)
    qvals = queries.astype(jnp.float32)
    state = step * qvals
    for index in range(ITERS):
        state = state + step * (qvals - jnp.dot(state, oper, precision=lax.Precision.HIGHEST))
    prepared = state.astype(jnp.bfloat16)
    blocks = train_grads.reshape(N_GRP * N_DEV, ROWS_DEV, K)

    def one_block(rows_block):
        return lax.dot_general(rows_block, prepared, (((1,), (1,)), ((), ())), preferred_element_type=jnp.float32).astype(jnp.bfloat16)

    return lax.map(one_block, blocks).reshape(TOTAL, QTOT)
```

```python
import jax
import jax.numpy as jnp
from jax import lax
from jax.experimental import pallas as pl
from jax.experimental.pallas import tpu as pltpu
from jax.sharding import PartitionSpec as P

MESH = pl.DeviceIdType.MESH
F32, BF16 = jnp.float32, jnp.bfloat16
ITERS = 8
DAMPING = 0.1
K = 1024
ROWS = 128
NB = K // 128
NX = NY = 4
NZ = 16
OWNED = ((0, 3, 4, 7), (1, 2, 5, 6))
SLOTS = {}
for _core, _rows in enumerate(OWNED):
    for _slot, _ij in enumerate((i, j) for i in _rows for j in range(i, NB)):
        SLOTS[_ij] = (_core, _slot)
NSLOT = 18
HELD = NSLOT * 128
HALF = HELD // 2
BIG = HALF // 4
SMALL = BIG // 4
TILES = 2 * SMALL // 8
CUT_BIG = (0, 144, 288)
CUT_SMALL = (0, 40, 72)
NSEM = 256


def split3(value):
    first = value.astype(BF16)
    rest = value - first.astype(F32)
    second = rest.astype(BF16)
    third = (rest - second.astype(F32)).astype(BF16)
    return first, second, third


def nt_dot(left, right):
    return lax.dot_general(left, right, (((1,), (1,)), ((), ())), preferred_element_type=F32)


def kernel(
    t_hbm, q_hbm, out_ref,
    tt, qb, part, held, r1, r2, s1, s2, zr, zr2, g0, g1, g2, colsum, xs, ys, pa,
    send_sem, recv_sem, local_sem,
):
    grp, dev = lax.axis_index("grp"), lax.axis_index("dev")
    y, zh, core = grp // 4, (grp // 2) % 2, grp % 2
    x, z = dev % 4, zh * 8 + dev // 4

    def where(px, py, pz, pc):
        return (py * 4 + (pz // 8) * 2 + pc, (pz % 8) * 4 + px)

    other = where(x, y, z, 1 - core)
    xp, xm = where((x + 1) % 4, y, z, core), where((x + 3) % 4, y, z, core)
    yp, ym = where(x, (y + 1) % 4, z, core), where(x, (y + 3) % 4, z, core)
    zs = [where(x, y, (z + d) % NZ, core) for d in range(NZ)]
    far = where(x, y, (z + 8) % NZ, core)

    started = []
    used = [0]

    def sems(n=1):
        base = used[0]
        used[0] += n
        assert used[0] <= NSEM
        return base

    def copy(src, dst, device, send, recv):
        return pltpu.make_async_remote_copy(
            src_ref=src, dst_ref=dst, send_sem=send_sem.at[send], recv_sem=recv_sem.at[recv],
            device_id=device, device_id_type=MESH,
        )

    def push(src, dst, device, send, recv=None):
        made = copy(src, dst, device, send, send if recv is None else recv)
        made.start()
        started.append(made)
        return made

    barrier = pltpu.get_barrier_semaphore()
    peers = [other, xp, xm, yp, ym] + zs[1:]
    for peer in peers:
        pl.semaphore_signal(barrier, inc=1, device_id=peer, device_id_type=MESH)
    mine_t = tt.at[pl.ds(pl.multiple_of(core * ROWS, ROWS), ROWS)]
    load_t = pltpu.make_async_copy(t_hbm, mine_t, local_sem.at[0])
    load_q = pltpu.make_async_copy(
        q_hbm.at[pl.ds(pl.multiple_of(x * 32, 32), 32)], qb.at[zh], local_sem.at[1]
    )
    load_t.start()
    load_q.start()
    load_t.wait()
    load_q.wait()
    pl.semaphore_wait(barrier, len(peers))

    send_t = push(mine_t, mine_t, other, sems())
    send_q = push(qb.at[zh], qb.at[zh], far, sems())
    send_t.wait_recv()

    def gram_rows(rows, cols):
        left = tt[:, rows * 128 : (rows + 1) * 128]
        right = tt[:, cols[0] * 128 : (cols[-1] + 1) * 128]
        return lax.dot_general(left, right, (((0,), (0,)), ((), ())), preferred_element_type=F32)

    for which in (0, 1):

        @pl.when(core == which)
        def _():
            for i in OWNED[which]:
                cols = list(range(i, NB))
                block = gram_rows(i, cols)
                for at, j in enumerate(cols):
                    slot = SLOTS[i, j][1]
                    part[slot * 128 : (slot + 1) * 128, :] = block[:, at * 128 : (at + 1) * 128]

    class Reduce:
        def __init__(self, base, cut, at, plus, minus, recv1, recv2, color):
            self.base, self.cut, self.at, self.plus, self.minus = base, cut, at, plus, minus
            self.r1, self.r2 = recv1, recv2
            self.color, self.sem = color, sems(6)
            self.moves = {}

        def piece(self, which, half):
            lo, hi = self.cut[half], self.cut[half + 1]
            row = self.base + which * self.cut[2] + lo
            return part.at[pl.ds(pl.multiple_of(row, 8), hi - lo)]

        def first(self, side):
            half = side
            return self.r1.at[self.color, side, pl.ds(0, self.cut[half + 1] - self.cut[half])]

        def second(self, side, half):
            lo, hi = self.cut[half], self.cut[half + 1]
            return self.r2.at[self.color, side, pl.ds(lo, hi - lo)]

        def start(self):
            a, s = self.at, self.sem
            self.moves[0] = push(self.piece((a + 2) % 4, 0), self.first(0), self.plus, s)
            self.moves[1] = push(self.piece((a + 2) % 4, 1), self.first(1), self.minus, s + 1)
            self.moves[2] = push(self.piece((a + 1) % 4, 1), self.second(0, 1), self.plus, s + 2)
            self.moves[3] = push(self.piece((a + 3) % 4, 0), self.second(1, 0), self.minus, s + 3)

        def middle(self):
            a, s = self.at, self.sem
            self.moves[0].wait_recv()
            mine = self.piece((a + 1) % 4, 0)
            mine[...] = mine[...] + self.first(0)[...]
            self.moves[1].wait_recv()
            mine1 = self.piece((a + 3) % 4, 1)
            mine1[...] = mine1[...] + self.first(1)[...]
            self.moves[4] = push(mine, self.second(0, 0), self.plus, s + 4)
            self.moves[5] = push(mine1, self.second(1, 1), self.minus, s + 5)

        def finish(self):
            for n in (2, 3, 4, 5):
                self.moves[n].wait_recv()
            row = self.base + self.at * self.cut[2]
            mine = part.at[pl.ds(pl.multiple_of(row, 8), self.cut[2])]
            total = mine[...] + self.r2[self.color, 0] + self.r2[self.color, 1]
            return mine, total

    base_a, base_b = 0, HALF
    red = [
        Reduce(base_a, CUT_BIG, x, xp, xm, r1, r2, 0),
        Reduce(base_b, CUT_BIG, y, yp, ym, r1, r2, 1),
    ]
    for r in red:
        r.start()
    for r in red:
        r.middle()
    for r in red:
        mine, total = r.finish()
        mine[...] = total
    red = [
        Reduce(base_a + x * BIG, CUT_SMALL, y, yp, ym, s1, s2, 0),
        Reduce(base_b + y * BIG, CUT_SMALL, x, xp, xm, s1, s2, 1),
    ]
    for r in red:
        r.start()
    for r in red:
        r.middle()
    off_a = base_a + x * BIG + y * SMALL
    off_b = base_b + y * BIG + x * SMALL
    for r in red:
        mine, total = r.finish()
        mine[...] = total

    def row_of(tile):
        late = tile // 9
        row = (1 - late) * (off_a + tile * 8) + late * (off_b + (tile - 9) * 8)
        return pl.multiple_of(row, 8)

    def tile_of(ref, tile):
        return ref.at[pl.ds(row_of(tile), 8)]

    my_held = held.at[core]
    sz_send, sz_recv = sems(NZ), sems(NZ)
    sz2_send, sz2_recv = sems(NZ), sems(NZ)
    late_sends = []
    for d in range(1, NZ):
        dest = (z + d) % NZ
        push(tile_of(part, dest), zr.at[z], zs[d], sz_send + d, sz_recv + z)
    for d in range(1, NZ):
        dest = (z + d) % NZ

        @pl.when(dest < TILES - NZ)
        def _():
            copy(tile_of(part, dest + NZ), zr2.at[z], zs[d], sz2_send + d, sz2_recv + z).start()

    zr[z] = part[pl.ds(row_of(z), 8), :]
    for d in range(1, NZ):
        src = (z + NZ - d) % NZ
        copy(zr.at[src], zr.at[src], zs[d], sz_send + d, sz_recv + src).wait_recv()
    total = zr[0]
    for n in range(1, NZ):
        total = total + zr[n]
    my_held[pl.ds(row_of(z), 8), :] = total

    @pl.when(z < TILES - NZ)
    def _():
        zr2[z] = part[pl.ds(row_of(z + NZ), 8), :]
        for d in range(1, NZ):
            src = (z + NZ - d) % NZ
            copy(zr2.at[src], zr2.at[src], zs[d], sz2_send + d, sz2_recv + src).wait_recv()
        total = zr2[0]
        for n in range(1, NZ):
            total = total + zr2[n]
        my_held[pl.ds(row_of(z + NZ), 8), :] = total

    gz_send, gz_recv = sems(NZ), sems(NZ)
    gz2_send, gz2_recv = sems(NZ), sems(TILES - NZ)
    mine = tile_of(my_held, z)
    for d in range(1, NZ):
        push(mine, mine, zs[d], gz_send + d, gz_recv + z)

    @pl.when(z < TILES - NZ)
    def _():
        mine = tile_of(my_held, z + NZ)
        for d in range(1, NZ):
            copy(mine, mine, zs[d], gz2_send + d, gz2_recv + z).start()

    for d in range(1, NZ):
        src = (z + NZ - d) % NZ
        got = tile_of(my_held, src)
        copy(got, got, zs[d], gz_send + d, gz_recv + src).wait_recv()
    for n in range(TILES - NZ):

        @pl.when(z != n)
        def _():
            got = tile_of(my_held, n + NZ)
            copy(got, got, zs[1], gz2_send + 1, gz2_recv + n).wait_recv()

    class Gather:
        def __init__(self, get, at, plus, minus):
            self.get, self.at, self.plus, self.minus, self.sem = get, at, plus, minus, sems(6)

        def start(self):
            g, a, s = self.get, self.at, self.sem
            push(g(a, 0), g(a, 0), self.plus, s)
            push(g(a, 1), g(a, 1), self.minus, s + 2)
            push(g(a, 1), g(a, 1), self.plus, s + 1)
            push(g(a, 0), g(a, 0), self.minus, s + 3)

        def got(self, which, half, n):
            ref = self.get(which % 4, half)
            copy(ref, ref, self.plus, self.sem + n, self.sem + n).wait_recv()
            return ref

        def middle(self):
            a, s = self.at, self.sem
            ref = self.got(a + 3, 0, 0)
            push(ref, ref, self.plus, s + 4)
            ref = self.got(a + 1, 1, 2)
            push(ref, ref, self.minus, s + 5)

        def near(self):
            self.got(self.at + 3, 1, 1)
            self.got(self.at + 1, 0, 3)

        def finish(self):
            self.got(self.at + 2, 0, 4)
            self.got(self.at + 2, 1, 5)

    def rows(base, cut):
        def get(which, half):
            lo, hi = cut[half], cut[half + 1]
            return my_held.at[pl.ds(pl.multiple_of(base + which * cut[2] + lo, 8), hi - lo)]

        return get

    def both(gathers):
        for g in gathers:
            g.start()
        for g in gathers:
            g.middle()

    pair = []

    def hand_over(ref):
        pair.append(push(ref, ref, other, sems()))

    stage = [
        Gather(rows(base_a + x * BIG, CUT_SMALL), y, yp, ym),
        Gather(rows(base_b + y * BIG, CUT_SMALL), x, xp, xm),
    ]
    both(stage)
    for g in stage:
        g.near()
        g.finish()

    def big(base, which):
        return my_held.at[pl.ds(pl.multiple_of(base + (which % 4) * BIG, 8), BIG)]

    bases = ((base_a, x), (base_b, y))
    stage = [
        Gather(rows(base_a, CUT_BIG), x, xp, xm),
        Gather(rows(base_b, CUT_BIG), y, yp, ym),
    ]
    both(stage)
    for base, a in bases:
        hand_over(big(base, a))
    for g, (base, a) in zip(stage, bases):
        g.near()
        hand_over(big(base, a + 3))
        hand_over(big(base, a + 1))
    for g, (base, a) in zip(stage, bases):
        g.finish()
        hand_over(big(base, a + 2))
    for made in pair:
        made.wait_recv()

    colsum[...] = jnp.zeros_like(colsum)
    trace = jnp.zeros((8, 128), F32)
    row_id = lax.broadcasted_iota(jnp.int32, (128, 128), 0)
    col_id = lax.broadcasted_iota(jnp.int32, (128, 128), 1)

    def place(block, i, j):
        at = (slice(i * 128, (i + 1) * 128), slice(j * 128, (j + 1) * 128))
        for plane, value in zip((g0, g1, g2), split3(block)):
            plane[at] = value
        colsum[:, at[1]] += jnp.sum(jnp.abs(block).reshape(16, 8, 128), axis=0)

    for i in range(NB):
        for j in range(i, NB):
            owner, slot = SLOTS[i, j]
            block = held[owner, slot * 128 : (slot + 1) * 128, :]
            place(block, i, j)
            if i == j:
                diag = jnp.where(row_id == col_id, block, 0.0)
                trace = trace + jnp.sum(diag.reshape(16, 8, 128), axis=0)
            else:
                place(block.T, j, i)

    total_rows = ROWS * lax.axis_size("grp") * lax.axis_size("dev")
    scale = 1.0 / total_rows
    trace = jnp.sum(jnp.sum(trace, axis=0, keepdims=True), axis=1, keepdims=True)
    damp = DAMPING * trace / (total_rows * K)
    sums = jnp.sum(colsum[...], axis=0, keepdims=True) * scale
    bound = jnp.max(sums, axis=1, keepdims=True) + damp
    step = 1.0 / bound

    send_q.wait_recv()

    def queries():
        return jnp.concatenate([qb[0], qb[1]], axis=0).astype(F32)

    ys[...] = step * queries()

    def iterate(_, carry):
        for n, value in enumerate(split3(ys[...])):
            xs[n * 64 : (n + 1) * 64, :] = value
        for n in range(4):
            at = slice(n * 256, (n + 1) * 256)
            low = jnp.dot(xs[0:64], g2[:, at], preferred_element_type=F32)
            mid = jnp.dot(xs[0:128], g1[:, at], preferred_element_type=F32)
            top = jnp.dot(xs[...], g0[:, at], preferred_element_type=F32)
            prod = top[0:64] + (top[64:128] + mid[0:64] + (top[128:192] + mid[64:128] + low))
            state = ys[:, at]
            query = jnp.concatenate([qb[0, :, at], qb[1, :, at]], axis=0).astype(F32)
            ys[:, at] = state + step * (query - (prod * scale + damp * state))
        return carry

    lax.fori_loop(0, ITERS, iterate, 0)
    pa[y, 0, core, x] = ys[0:32, :].astype(BF16)
    pa[y, 1, core, x] = ys[32:64, :].astype(BF16)

    pair = []
    hand_over(pa.at[y, 0, core, x])
    hand_over(pa.at[y, 1, core, x])
    stage = [
        Gather(lambda p, h: pa.at[y, 0, core, p, pl.ds(16 * h, 16)], x, xp, xm),
        Gather(lambda p, h: pa.at[p, 1, core, x, pl.ds(16 * h, 16)], y, yp, ym),
    ]
    both(stage)
    for g in stage:
        g.near()
        g.finish()
    stage = [
        Gather(lambda p, h: pa.at[p, 0, core, pl.ds(2 * h, 2)], y, yp, ym),
        Gather(lambda p, h: pa.at[pl.ds(2 * h, 2), 1, core, p], x, xp, xm),
    ]
    both(stage)
    for n in range(1, 4):
        hand_over(pa.at[y, 0, core, (x + n) % 4])
        hand_over(pa.at[(y + n) % 4, 1, core, x])
    for g in stage:
        g.near()
    for n in (3, 1):
        hand_over(pa.at[(y + n) % 4, 0, core])
        hand_over(pa.at[:, 1, core, (x + n) % 4])
    for g in stage:
        g.finish()
    hand_over(pa.at[(y + 2) % 4, 0, core])
    hand_over(pa.at[:, 1, core, (x + 2) % 4])
    for made in pair:
        made.wait_recv()

    own = tt[pl.ds(pl.multiple_of(core * ROWS, ROWS), ROWS), :]
    for yy in range(4):
        for half in range(2):
            block = pa[yy, half].reshape(256, K)
            at = (yy * 2 + half) * 256
            out_ref[:, at : at + 256] = nt_dot(own, block).astype(BF16)

    for made in started:
        made.wait_send()
    for d in range(1, NZ):
        dest = (z + d) % NZ

        @pl.when(dest < TILES - NZ)
        def _():
            copy(tile_of(part, dest + NZ), zr2.at[z], zs[d], sz2_send + d, sz2_recv + z).wait_send()

        @pl.when(z < TILES - NZ)
        def _():
            mine = tile_of(my_held, z + NZ)
            copy(mine, mine, zs[d], gz2_send + d, gz2_recv + z).wait_send()


def body(train_grads, queries):
    nquery = queries.shape[0] * lax.axis_size("grp")
    return pl.pallas_call(
        kernel,
        out_shape=jax.ShapeDtypeStruct((ROWS, nquery), BF16),
        in_specs=[pl.BlockSpec(memory_space=pl.ANY)] * 2,
        out_specs=pl.BlockSpec(memory_space=pltpu.VMEM),
        scratch_shapes=[
            pltpu.VMEM((2 * ROWS, K), BF16),
            pltpu.VMEM((2, 32, K), BF16),
            pltpu.VMEM((HELD, 128), F32),
            pltpu.VMEM((2, HELD, 128), F32),
            pltpu.VMEM((2, 2, BIG // 2, 128), F32),
            pltpu.VMEM((2, 2, BIG, 128), F32),
            pltpu.VMEM((2, 2, CUT_SMALL[1], 128), F32),
            pltpu.VMEM((2, 2, SMALL, 128), F32),
            pltpu.VMEM((NZ, 8, 128), F32),
            pltpu.VMEM((NZ, 8, 128), F32),
            pltpu.VMEM((K, K), BF16),
            pltpu.VMEM((K, K), BF16),
            pltpu.VMEM((K, K), BF16),
            pltpu.VMEM((8, K), F32),
            pltpu.VMEM((192, K), BF16),
            pltpu.VMEM((64, K), F32),
            pltpu.VMEM((4, 2, 2, 4, 32, K), BF16),
            pltpu.SemaphoreType.DMA((NSEM,)),
            pltpu.SemaphoreType.DMA((NSEM,)),
            pltpu.SemaphoreType.DMA((2,)),
        ],
        compiler_params=pltpu.CompilerParams(
            collective_id=0, has_side_effects=True, vmem_limit_bytes=48 * 1024 * 1024
        ),
    )(train_grads, queries)


def solution(mesh):
    return jax.shard_map(
        body,
        mesh=mesh,
        in_specs=(P(("grp", "dev"), None), P("grp", None)),
        out_specs=P(("grp", "dev"), None),
        check_vma=False,
    )
```

```python
import jax
import jax.numpy as jnp
from jax import lax
from jax.experimental import pallas as pl
from jax.experimental.pallas import tpu as pltpu
from jax.sharding import PartitionSpec as P

MESH = pl.DeviceIdType.MESH
F32, BF16 = jnp.float32, jnp.bfloat16
ITERS = 8
DAMPING = 0.1
K = 1024
ROWS = 128
NB = K // 128
NX = NY = 4
NZ = 16
OWNED = ((0, 3, 4, 7), (1, 2, 5, 6))
SLOTS = {}
for _core, _rows in enumerate(OWNED):
    for _slot, _ij in enumerate((i, j) for i in _rows for j in range(i, NB)):
        SLOTS[_ij] = (_core, _slot)
NSLOT = 18
HELD = NSLOT * 128
HALF = HELD // 2
BIG = HALF // 4
SMALL = BIG // 4
TILES = 2 * SMALL // 8
CUT_BIG = (0, 144, 288)
CUT_SMALL = (0, 40, 72)
NSEM = 320
FAR_FIRST = sorted(range(1, NZ), key=lambda d: -min(d, NZ - d))


def split3(value):
    first = value.astype(BF16)
    rest = value - first.astype(F32)
    second = rest.astype(BF16)
    third = (rest - second.astype(F32)).astype(BF16)
    return first, second, third


def nt_dot(left, right):
    return lax.dot_general(left, right, (((1,), (1,)), ((), ())), preferred_element_type=F32)


def kernel(
    t_hbm, q_hbm, out_hbm,
    tt, tq, qv, qb, part, held, r1, r2, r3, zr, zr2, g0, g1, rest, colsum, xs, ys, pa, ob,
    send_sem, recv_sem, local_sem,
):
    grp, dev = lax.axis_index("grp"), lax.axis_index("dev")
    y, zh, core = grp // 4, (grp // 2) % 2, grp % 2
    x, z = dev % 4, zh * 8 + dev // 4

    def where(px, py, pz, pc):
        return (py * 4 + (pz // 8) * 2 + pc, (pz % 8) * 4 + px)

    other = where(x, y, z, 1 - core)
    xp, xm = where((x + 1) % 4, y, z, core), where((x + 3) % 4, y, z, core)
    yp, ym = where(x, (y + 1) % 4, z, core), where(x, (y + 3) % 4, z, core)
    xo, yo = where((x + 2) % 4, y, z, core), where(x, (y + 2) % 4, z, core)
    zs = [where(x, y, (z + d) % NZ, core) for d in range(NZ)]
    odd = z % 2
    neighbour = where(x, y, z + 1 - 2 * odd, core)
    near_half = (zh + odd) % 2
    far = where(x, y, (z + 8) % NZ, core)

    started = []
    used = [0]

    def sems(n=1):
        base = used[0]
        used[0] += n
        assert used[0] <= NSEM
        return base

    def copy(src, dst, device, send, recv):
        return pltpu.make_async_remote_copy(
            src_ref=src, dst_ref=dst, send_sem=send_sem.at[send], recv_sem=recv_sem.at[recv],
            device_id=device, device_id_type=MESH,
        )

    def push(src, dst, device, send, recv=None):
        made = copy(src, dst, device, send, send if recv is None else recv)
        made.start()
        started.append(made)
        return made

    barrier = pltpu.get_barrier_semaphore()
    peers = [other, xp, xm, xo, yp, ym, yo] + zs[1:]
    for peer in peers:
        pl.semaphore_signal(barrier, inc=1, device_id=peer, device_id_type=MESH)
    mine_t = tt.at[pl.ds(pl.multiple_of(core * ROWS, ROWS), ROWS)]
    load_t = pltpu.make_async_copy(t_hbm, mine_t, local_sem.at[0])
    load_q = pltpu.make_async_copy(q_hbm, qv, local_sem.at[1])
    load_own = pltpu.make_async_copy(t_hbm, tq.at[pl.ds(0, ROWS)], local_sem.at[2])
    load_t.start()
    load_q.start()
    load_own.start()
    load_t.wait()
    pl.semaphore_wait(barrier, len(peers))

    send_t = push(mine_t, mine_t, other, sems())
    send_near = push(mine_t, tq.at[pl.ds(ROWS, ROWS)], neighbour, sems())
    send_t.wait_recv()

    def gram_rows(rows, cols):
        left = tt[:, rows * 128 : (rows + 1) * 128]
        right = tt[:, cols[0] * 128 : (cols[-1] + 1) * 128]
        return lax.dot_general(left, right, (((0,), (0,)), ((), ())), preferred_element_type=F32)

    for which in (0, 1):

        @pl.when(core == which)
        def _():
            for i in OWNED[which]:
                cols = list(range(i, NB))
                block = gram_rows(i, cols)
                for at, j in enumerate(cols):
                    slot = SLOTS[i, j][1]
                    part[slot * 128 : (slot + 1) * 128, :] = block[:, at * 128 : (at + 1) * 128]

    class Reduce:
        def __init__(self, base, cut, at, plus, minus, recv1, recv2, color):
            self.base, self.cut, self.at, self.plus, self.minus = base, cut, at, plus, minus
            self.r1, self.r2 = recv1, recv2
            self.color, self.sem = color, sems(6)
            self.moves = {}

        def piece(self, which, half):
            lo, hi = self.cut[half], self.cut[half + 1]
            row = self.base + which * self.cut[2] + lo
            return part.at[pl.ds(pl.multiple_of(row, 8), hi - lo)]

        def first(self, side):
            half = side
            return self.r1.at[self.color, side, pl.ds(0, self.cut[half + 1] - self.cut[half])]

        def second(self, side, half):
            lo, hi = self.cut[half], self.cut[half + 1]
            return self.r2.at[self.color, side, pl.ds(lo, hi - lo)]

        def start(self):
            a, s = self.at, self.sem
            self.moves[0] = push(self.piece((a + 2) % 4, 0), self.first(0), self.plus, s)
            self.moves[1] = push(self.piece((a + 2) % 4, 1), self.first(1), self.minus, s + 1)
            self.moves[2] = push(self.piece((a + 1) % 4, 1), self.second(0, 1), self.plus, s + 2)
            self.moves[3] = push(self.piece((a + 3) % 4, 0), self.second(1, 0), self.minus, s + 3)

        def middle(self):
            a, s = self.at, self.sem
            self.moves[0].wait_recv()
            mine = self.piece((a + 1) % 4, 0)
            mine[...] = mine[...] + self.first(0)[...]
            self.moves[1].wait_recv()
            mine1 = self.piece((a + 3) % 4, 1)
            mine1[...] = mine1[...] + self.first(1)[...]
            self.moves[4] = push(mine, self.second(0, 0), self.plus, s + 4)
            self.moves[5] = push(mine1, self.second(1, 1), self.minus, s + 5)

        def finish(self):
            for n in (2, 3, 4, 5):
                self.moves[n].wait_recv()
            row = self.base + self.at * self.cut[2]
            mine = part.at[pl.ds(pl.multiple_of(row, 8), self.cut[2])]
            total = mine[...] + self.r2[self.color, 0] + self.r2[self.color, 1]
            return mine, total

    base_a, base_b = 0, HALF
    red = [
        Reduce(base_a, CUT_BIG, x, xp, xm, r1, r2, 0),
        Reduce(base_b, CUT_BIG, y, yp, ym, r1, r2, 1),
    ]
    for r in red:
        r.start()
    for r in red:
        r.middle()
    for r in red:
        mine, total = r.finish()
        mine[...] = total
    off_a = base_a + x * BIG + y * SMALL
    off_b = base_b + y * BIG + x * SMALL
    colors = (
        (base_a + x * BIG, y, (None, yp, yo, ym), off_a),
        (base_b + y * BIG, x, (None, xp, xo, xm), off_b),
    )
    cross = [sems(4), sems(4)]
    moves = []
    for n in (2, 1, 3):
        for color, (base, a, peer, _) in enumerate(colors):
            row = pl.multiple_of(base + ((a + n) % 4) * SMALL, 8)
            moves.append(push(part.at[pl.ds(row, SMALL)], r3.at[color, n], peer[n], cross[color] + n))
    for made in moves:
        made.wait_recv()
    for color, (base, a, peer, off) in enumerate(colors):
        mine = part.at[pl.ds(pl.multiple_of(off, 8), SMALL)]
        mine[...] = (mine[...] + r3[color, 2]) + (r3[color, 1] + r3[color, 3])

    load_q.wait()
    load_own.wait()

    def chunk(at):
        return qv.at[pl.ds(pl.multiple_of(at * 32, 32), 32)]

    sem_q = sems(4)
    source = (core == 1) & (x == y)
    receiver = (core == 1) & (x != y)

    @pl.when(jnp.logical_not(receiver))
    def _():
        qb[0] = qv[pl.ds(pl.multiple_of(x * 32, 32), 32), :]

    row_peers = (None, yp, yo, ym)
    for d in (1, 2, 3):

        @pl.when(source)
        def _():
            copy(chunk((y + d) % 4), qb.at[0], row_peers[d], sem_q + d, sem_q).start()

    def row_of(tile):
        late = tile // 9
        row = (1 - late) * (off_a + tile * 8) + late * (off_b + (tile - 9) * 8)
        return pl.multiple_of(row, 8)

    def tile_of(ref, tile):
        return ref.at[pl.ds(row_of(tile), 8)]

    my_held = held.at[core]
    sz, sz2 = sems(NZ), sems(NZ)
    for d in FAR_FIRST:
        dest = (z + d) % NZ
        push(tile_of(part, dest), zr.at[z], zs[d], sz + d, sz + z)
    for d in FAR_FIRST:
        dest = (z + d) % NZ

        @pl.when(dest < TILES - NZ)
        def _():
            copy(tile_of(part, dest + NZ), zr2.at[z], zs[d], sz2 + d, sz2 + z).start()

    zr[z] = part[pl.ds(row_of(z), 8), :]
    for d in FAR_FIRST:
        src = (z + NZ - d) % NZ
        copy(zr.at[src], zr.at[src], zs[d], sz + d, sz + src).wait_recv()
    total = zr[0]
    for n in range(1, NZ):
        total = total + zr[n]
    my_held[pl.ds(row_of(z), 8), :] = total

    @pl.when(z < TILES - NZ)
    def _():
        zr2[z] = part[pl.ds(row_of(z + NZ), 8), :]
        for d in FAR_FIRST:
            src = (z + NZ - d) % NZ
            copy(zr2.at[src], zr2.at[src], zs[d], sz2 + d, sz2 + src).wait_recv()
        total = zr2[0]
        for n in range(1, NZ):
            total = total + zr2[n]
        my_held[pl.ds(row_of(z + NZ), 8), :] = total

    gz, gz2 = sems(NZ), sems(NZ)
    mine = tile_of(my_held, z)
    for d in FAR_FIRST:
        push(mine, mine, zs[d], gz + d, gz + z)

    @pl.when(z < TILES - NZ)
    def _():
        mine = tile_of(my_held, z + NZ)
        for d in FAR_FIRST:
            copy(mine, mine, zs[d], gz2 + d, gz2 + z).start()

    for d in FAR_FIRST:
        src = (z + NZ - d) % NZ
        got = tile_of(my_held, src)
        copy(got, got, zs[d], gz + d, gz + src).wait_recv()
    for n in range(TILES - NZ):

        @pl.when(z != n)
        def _():
            got = tile_of(my_held, n + NZ)
            copy(got, got, zs[1], gz2 + 1, gz2 + n).wait_recv()

    class Gather:
        def __init__(self, get, whole, f, s, first, second):
            self.get, self.whole, self.f, self.s = get, whole, f, s
            self.first, self.second = first, second
            self.first_sem = sems(4)
            self.second_sem = [sems(6) for _ in range(4)]
            self.pair = sems(16)

        def chunk(self, n, m, half=None):
            at = (self.f + n) % 4, (self.s + m) % 4
            return self.whole(*at) if half is None else self.get(*at, half)

        def wait(self, ref, sem):
            copy(ref, ref, other, sem, sem).wait_recv()

        def start(self):
            mine = self.chunk(0, 0)
            for n in (1, 3, 2):
                push(mine, mine, self.first[n - 1], self.first_sem + n)

        def landed(self, n):
            self.wait(self.chunk(n, 0), self.first_sem + 4 - n)

        def send(self, n):
            sem = self.second_sem[n]
            plus, across, minus = self.second
            for device, half, k in ((plus, 0, 0), (minus, 1, 2), (plus, 1, 1), (minus, 0, 3)):
                ref = self.chunk(n, 0, half)
                push(ref, ref, device, sem + k)
            if n == 2:
                ref = self.chunk(n, 0)
                push(ref, ref, across, sem + 4)

        def forward(self, n):
            sem = self.second_sem[n]
            plus, _, minus = self.second
            for m, half, k, device in ((3, 0, 0, plus), (1, 1, 2, minus)):
                ref = self.chunk(n, m, half)
                self.wait(ref, sem + k)
                if n != 2:
                    push(ref, ref, device, sem + 4 + half)

        def near(self, n):
            sem = self.second_sem[n]
            self.wait(self.chunk(n, 3, 1), sem + 1)
            self.wait(self.chunk(n, 1, 0), sem + 3)
            self.hand(n, 3)
            self.hand(n, 1)

        def last(self, n):
            sem = self.second_sem[n]
            if n == 2:
                self.wait(self.chunk(n, 2), sem + 4)
            else:
                self.wait(self.chunk(n, 2, 0), sem + 4)
                self.wait(self.chunk(n, 2, 1), sem + 5)
            self.hand(n, 2)

        def paired(self, n, m):
            return self.chunk(n, m), self.pair + n * 4 + m

        def hand(self, n, m):
            ref, sem = self.paired(n, m)
            push(ref, ref, other, sem)

        def handed(self, n):
            for m in range(4):
                self.wait(*self.paired(n, m))

    def gather(both, ready):
        for g in both:
            g.start()
        for g in both:
            g.send(0)
            g.hand(0, 0)
        for n in (3, 1):
            for g in both:
                g.landed(n)
                g.send(n)
                g.hand(n, 0)
        for g in both:
            g.forward(0)
        for g in both:
            g.landed(2)
            g.send(2)
            g.hand(2, 0)
        for g in both:
            g.near(0)
        for g in both:
            g.forward(3)
        for g in both:
            g.last(0)
        for g in both:
            g.near(3)
        for g in both:
            g.forward(1)
        ready(0)
        for g in both:
            g.last(3)
        for g in both:
            g.near(1)
        ready(3)
        for g in both:
            g.last(1)
        ready(1)
        for g in both:
            g.forward(2)
            g.near(2)
        for g in both:
            g.last(2)
        ready(2)

    def held_rows(base):
        def get(f, s, half):
            lo, hi = CUT_SMALL[half], CUT_SMALL[half + 1]
            return my_held.at[pl.ds(pl.multiple_of(base + s * BIG + f * SMALL + lo, 8), hi - lo)]

        def whole(f, s):
            return my_held.at[pl.ds(pl.multiple_of(base + s * BIG + f * SMALL, 8), SMALL)]

        return get, whole

    sem_f = sems()

    @pl.when(receiver)
    def _():
        copy(qb.at[0], qb.at[0], yp, sem_q, sem_q).wait_recv()

    @pl.when(odd == 1)
    def _():
        copy(qb.at[0], qb.at[1], far, sem_f, sem_f).start()

    both = [
        Gather(*held_rows(base_a), y, x, (yp, yo, ym), (xp, xo, xm)),
        Gather(*held_rows(base_b), x, y, (xp, xo, xm), (yp, yo, ym)),
    ]
    gather(both, lambda n: None)
    for n in range(4):
        for g in both:
            g.handed(n)

    colsum[...] = jnp.zeros_like(colsum)
    trace = jnp.zeros((8, 128), F32)
    row_id = lax.broadcasted_iota(jnp.int32, (128, 128), 0)
    col_id = lax.broadcasted_iota(jnp.int32, (128, 128), 1)

    def place(block, i, j):
        at = (slice(i * 128, (i + 1) * 128), slice(j * 128, (j + 1) * 128))
        first = block.astype(BF16)
        left = block - first.astype(F32)
        second = left.astype(BF16)
        g0[at] = first
        g1[at] = second
        if i == j:
            third = jnp.where(row_id == col_id, left - second.astype(F32), 0.0)
            rest[:, at[1]] = jnp.sum(third, axis=0, keepdims=True)
        colsum[:, at[1]] += jnp.sum(jnp.abs(block).reshape(16, 8, 128), axis=0)

    for i in range(NB):
        for j in range(i, NB):
            owner, slot = SLOTS[i, j]
            block = held[owner, slot * 128 : (slot + 1) * 128, :]
            place(block, i, j)
            if i == j:
                diag = jnp.where(row_id == col_id, block, 0.0)
                trace = trace + jnp.sum(diag.reshape(16, 8, 128), axis=0)
            else:
                place(block.T, j, i)

    total_rows = ROWS * lax.axis_size("grp") * lax.axis_size("dev")
    scale = 1.0 / total_rows
    trace = jnp.sum(jnp.sum(trace, axis=0, keepdims=True), axis=1, keepdims=True)
    damp = DAMPING * trace / (total_rows * K)
    sums = jnp.sum(colsum[...], axis=0, keepdims=True) * scale
    bound = jnp.max(sums, axis=1, keepdims=True) + damp
    step = 1.0 / bound

    @pl.when(odd == 1)
    def _():
        copy(qb.at[0], qb.at[1], far, sem_f, sem_f).wait_recv()

    ys[...] = step * qb[odd].astype(F32)

    def iterate(_, carry):
        for n, value in enumerate(split3(ys[...])):
            xs[n * 32 : (n + 1) * 32, :] = value
        for n in range(4):
            at = slice(n * 256, (n + 1) * 256)
            mid = jnp.dot(xs[0:64], g1[:, at], preferred_element_type=F32)
            top = jnp.dot(xs[...], g0[:, at], preferred_element_type=F32)
            state = ys[:, at]
            prod = top[0:32] + (top[32:64] + mid[0:32] + (top[64:96] + mid[32:64] + state * rest[:, at]))
            query = qb[odd, :, at].astype(F32)
            ys[:, at] = state + step * (query - (prod * scale + damp * state))
        return carry

    lax.fori_loop(0, ITERS, iterate, 0)

    first_at, second_at = (1 - core) * y + core * x, (1 - core) * x + core * y

    def along(step, first):
        dx = step * (core if first else 1 - core)
        dy = step * (1 - core if first else core)
        return where((x + dx) % 4, (y + dy) % 4, z, core)

    pa[core, first_at, second_at] = ys[...].astype(BF16)

    out_sem = sems(8)
    send_near.wait_recv()
    kept = []

    def scores(far, n):
        which = (1 - far) * core + far * (1 - core)
        block = ((second_at if far else first_at) + n) % 4
        slot = far * 4 + n
        found = nt_dot(tq[...], pa[which, block].reshape(128, K)).astype(BF16)
        ob[slot, 0] = found[0:ROWS]
        ob[slot, 1] = found[ROWS : 2 * ROWS]
        col = pl.multiple_of((block * 4 + near_half * 2 + which) * 128, 128)
        push(ob.at[slot, 1], out_hbm.at[:, pl.ds(col, 128)], neighbour, out_sem + slot)
        keep = pltpu.make_async_copy(
            ob.at[slot, 0], out_hbm.at[:, pl.ds(col, 128)], local_sem.at[3 + slot]
        )
        keep.start()
        kept.append(keep)

    prepared = Gather(
        lambda f, s, h: pa.at[core, f, s, pl.ds(16 * h, 16)],
        lambda f, s: pa.at[core, f, s],
        first_at,
        second_at,
        [along(n, True) for n in (1, 2, 3)],
        [along(n, False) for n in (1, 2, 3)],
    )

    def handed(n):
        for m in range(4):
            ref = pa.at[1 - core, (second_at + n) % 4, (first_at + m) % 4]
            sem = prepared.pair + n * 4 + m
            copy(ref, ref, other, sem, sem).wait_recv()

    def ready(n):
        scores(0, n)
        if n in (3, 1):
            done = 0 if n == 3 else 3
            handed(done)
            scores(1, done)

    gather([prepared], ready)
    for n in (1, 2):
        handed(n)
        scores(1, n)
    for slot in range(8):
        far, n = slot // 4, slot % 4
        which = (1 - far) * core + far * (1 - core)
        block = ((second_at if far else first_at) + n) % 4
        col = pl.multiple_of((block * 4 + (1 - near_half) * 2 + which) * 128, 128)
        ref = out_hbm.at[:, pl.ds(col, 128)]
        copy(ob.at[slot, 1], ref, neighbour, out_sem + slot, out_sem + slot).wait_recv()

    for keep in kept:
        keep.wait()
    for made in started:
        made.wait_send()

    for d in (1, 2, 3):

        @pl.when(source)
        def _():
            copy(chunk((y + d) % 4), qb.at[0], row_peers[d], sem_q + d, sem_q).wait_send()

    @pl.when(odd == 1)
    def _():
        copy(qb.at[0], qb.at[1], far, sem_f, sem_f).wait_send()

    for d in FAR_FIRST:
        dest = (z + d) % NZ

        @pl.when(dest < TILES - NZ)
        def _():
            copy(tile_of(part, dest + NZ), zr2.at[z], zs[d], sz2 + d, sz2 + z).wait_send()

        @pl.when(z < TILES - NZ)
        def _():
            mine = tile_of(my_held, z + NZ)
            copy(mine, mine, zs[d], gz2 + d, gz2 + z).wait_send()


def body(train_grads, queries):
    nquery = queries.shape[0] * lax.axis_size("grp")
    return pl.pallas_call(
        kernel,
        out_shape=jax.ShapeDtypeStruct((ROWS, nquery), BF16),
        in_specs=[pl.BlockSpec(memory_space=pltpu.HBM)] * 2,
        out_specs=pl.BlockSpec(memory_space=pltpu.HBM),
        scratch_shapes=[
            pltpu.VMEM((2 * ROWS, K), BF16),
            pltpu.VMEM((2 * ROWS, K), BF16),
            pltpu.VMEM((ROWS, K), BF16),
            pltpu.VMEM((2, 32, K), BF16),
            pltpu.VMEM((HELD, 128), F32),
            pltpu.VMEM((2, HELD, 128), F32),
            pltpu.VMEM((2, 2, BIG // 2, 128), F32),
            pltpu.VMEM((2, 2, BIG, 128), F32),
            pltpu.VMEM((2, 4, SMALL, 128), F32),
            pltpu.VMEM((NZ, 8, 128), F32),
            pltpu.VMEM((NZ, 8, 128), F32),
            pltpu.VMEM((K, K), BF16),
            pltpu.VMEM((K, K), BF16),
            pltpu.VMEM((1, K), F32),
            pltpu.VMEM((8, K), F32),
            pltpu.VMEM((96, K), BF16),
            pltpu.VMEM((32, K), F32),
            pltpu.VMEM((2, 4, 4, 32, K), BF16),
            pltpu.VMEM((8, 2, ROWS, 128), BF16),
            pltpu.SemaphoreType.DMA((NSEM,)),
            pltpu.SemaphoreType.DMA((NSEM,)),
            pltpu.SemaphoreType.DMA((11,)),
        ],
        compiler_params=pltpu.CompilerParams(
            collective_id=0, has_side_effects=True, vmem_limit_bytes=63 * 1024 * 1024
        ),
    )(train_grads, queries)


def solution(mesh):
    return jax.shard_map(
        body,
        mesh=mesh,
        in_specs=(P(("grp", "dev"), None), P("grp", None)),
        out_specs=P(("grp", "dev"), None),
        check_vma=False,
    )
```

```python
import jax
import jax.numpy as jnp
from jax import lax
from jax.experimental import pallas as pl
from jax.experimental.pallas import tpu as pltpu
from jax.sharding import PartitionSpec as P

MESH = pl.DeviceIdType.MESH
F32, BF16 = jnp.float32, jnp.bfloat16
ITERS = 8
DAMPING = 0.1
K = 1024
ROWS = 128
NB = K // 128
NX = NY = 4
NZ = 16
OWNED = ((0, 3, 4, 7), (1, 2, 5, 6))
SLOTS = {}
for _core, _rows in enumerate(OWNED):
    for _slot, _ij in enumerate((i, j) for i in _rows for j in range(i, NB)):
        SLOTS[_ij] = (_core, _slot)
NSLOT = 18
HELD = NSLOT * 128
HALF = HELD // 2
BIG = HALF // 4
SMALL = BIG // 4
TILES = 2 * SMALL // 8
CUT_BIG = (0, 144, 288)
NSEM = 320
FAR_FIRST = sorted(range(1, NZ), key=lambda d: -min(d, NZ - d))


def split3(value):
    first = value.astype(BF16)
    rest = value - first.astype(F32)
    second = rest.astype(BF16)
    third = (rest - second.astype(F32)).astype(BF16)
    return first, second, third


def nt_dot(left, right):
    return lax.dot_general(left, right, (((1,), (1,)), ((), ())), preferred_element_type=F32)


def kernel(
    t_hbm, q_hbm, out_hbm,
    tt, tq, qv, qb, part, held, r1, r2, r3, zr, zr2, g0, g1, rest, colsum, trace, xs, ys, pa, ob,
    send_sem, recv_sem, local_sem,
):
    grp, dev = lax.axis_index("grp"), lax.axis_index("dev")
    y, zh, core = grp // 4, (grp // 2) % 2, grp % 2
    x, z = dev % 4, zh * 8 + dev // 4

    def where(px, py, pz, pc):
        return (py * 4 + (pz // 8) * 2 + pc, (pz % 8) * 4 + px)

    other = where(x, y, z, 1 - core)
    xp, xm = where((x + 1) % 4, y, z, core), where((x + 3) % 4, y, z, core)
    yp, ym = where(x, (y + 1) % 4, z, core), where(x, (y + 3) % 4, z, core)
    xo, yo = where((x + 2) % 4, y, z, core), where(x, (y + 2) % 4, z, core)
    zs = [where(x, y, (z + d) % NZ, core) for d in range(NZ)]
    odd = z % 2
    neighbour = where(x, y, z + 1 - 2 * odd, core)
    near_half = (zh + odd) % 2
    far = where(x, y, (z + 8) % NZ, core)

    started = []
    used = [0]

    def sems(n=1):
        base = used[0]
        used[0] += n
        assert used[0] <= NSEM
        return base

    def copy(src, dst, device, send, recv):
        return pltpu.make_async_remote_copy(
            src_ref=src, dst_ref=dst, send_sem=send_sem.at[send], recv_sem=recv_sem.at[recv],
            device_id=device, device_id_type=MESH,
        )

    def push(src, dst, device, send, recv=None):
        made = copy(src, dst, device, send, send if recv is None else recv)
        made.start()
        started.append(made)
        return made

    barrier = pltpu.get_barrier_semaphore()
    peers = [other, xp, xm, xo, yp, ym, yo] + zs[1:]
    for peer in peers:
        pl.semaphore_signal(barrier, inc=1, device_id=peer, device_id_type=MESH)
    mine_t = tt.at[pl.ds(pl.multiple_of(core * ROWS, ROWS), ROWS)]
    load_t = pltpu.make_async_copy(t_hbm, mine_t, local_sem.at[0])
    load_q = pltpu.make_async_copy(q_hbm, qv, local_sem.at[1])
    load_own = pltpu.make_async_copy(t_hbm, tq.at[pl.ds(0, ROWS)], local_sem.at[2])
    load_t.start()
    load_q.start()
    load_own.start()
    load_t.wait()
    pl.semaphore_wait(barrier, len(peers))

    send_t = push(mine_t, mine_t, other, sems())
    send_near = push(mine_t, tq.at[pl.ds(ROWS, ROWS)], neighbour, sems())
    send_t.wait_recv()

    def gram_rows(rows, cols):
        left = tt[:, rows * 128 : (rows + 1) * 128]
        right = tt[:, cols[0] * 128 : (cols[-1] + 1) * 128]
        return lax.dot_general(left, right, (((0,), (0,)), ((), ())), preferred_element_type=F32)

    for which in (0, 1):

        @pl.when(core == which)
        def _():
            for i in OWNED[which]:
                cols = list(range(i, NB))
                block = gram_rows(i, cols)
                for at, j in enumerate(cols):
                    slot = SLOTS[i, j][1]
                    part[slot * 128 : (slot + 1) * 128, :] = block[:, at * 128 : (at + 1) * 128]

    class Reduce:
        def __init__(self, base, cut, at, plus, minus, recv1, recv2, color):
            self.base, self.cut, self.at, self.plus, self.minus = base, cut, at, plus, minus
            self.r1, self.r2 = recv1, recv2
            self.color, self.sem = color, sems(6)
            self.moves = {}

        def piece(self, which, half):
            lo, hi = self.cut[half], self.cut[half + 1]
            row = self.base + which * self.cut[2] + lo
            return part.at[pl.ds(pl.multiple_of(row, 8), hi - lo)]

        def first(self, side):
            half = side
            return self.r1.at[self.color, side, pl.ds(0, self.cut[half + 1] - self.cut[half])]

        def second(self, side, half):
            lo, hi = self.cut[half], self.cut[half + 1]
            return self.r2.at[self.color, side, pl.ds(lo, hi - lo)]

        def start(self):
            a, s = self.at, self.sem
            self.moves[0] = push(self.piece((a + 2) % 4, 0), self.first(0), self.plus, s)
            self.moves[1] = push(self.piece((a + 2) % 4, 1), self.first(1), self.minus, s + 1)
            self.moves[2] = push(self.piece((a + 1) % 4, 1), self.second(0, 1), self.plus, s + 2)
            self.moves[3] = push(self.piece((a + 3) % 4, 0), self.second(1, 0), self.minus, s + 3)

        def middle(self):
            a, s = self.at, self.sem
            self.moves[0].wait_recv()
            mine = self.piece((a + 1) % 4, 0)
            mine[...] = mine[...] + self.first(0)[...]
            self.moves[1].wait_recv()
            mine1 = self.piece((a + 3) % 4, 1)
            mine1[...] = mine1[...] + self.first(1)[...]
            self.moves[4] = push(mine, self.second(0, 0), self.plus, s + 4)
            self.moves[5] = push(mine1, self.second(1, 1), self.minus, s + 5)

        def finish(self):
            for n in (2, 3, 4, 5):
                self.moves[n].wait_recv()
            row = self.base + self.at * self.cut[2]
            mine = part.at[pl.ds(pl.multiple_of(row, 8), self.cut[2])]
            total = mine[...] + self.r2[self.color, 0] + self.r2[self.color, 1]
            return mine, total

    base_a, base_b = 0, HALF
    red = [
        Reduce(base_a, CUT_BIG, x, xp, xm, r1, r2, 0),
        Reduce(base_b, CUT_BIG, y, yp, ym, r1, r2, 1),
    ]
    for r in red:
        r.start()
    for r in red:
        r.middle()
    for r in red:
        mine, total = r.finish()
        mine[...] = total
    off_a = base_a + x * BIG + y * SMALL
    off_b = base_b + y * BIG + x * SMALL
    colors = (
        (base_a + x * BIG, y, (None, yp, yo, ym), off_a),
        (base_b + y * BIG, x, (None, xp, xo, xm), off_b),
    )
    cross = [sems(4), sems(4)]
    moves = []
    for n in (2, 1, 3):
        for color, (base, a, peer, _) in enumerate(colors):
            row = pl.multiple_of(base + ((a + n) % 4) * SMALL, 8)
            moves.append(push(part.at[pl.ds(row, SMALL)], r3.at[color, n], peer[n], cross[color] + n))
    for made in moves:
        made.wait_recv()
    for color, (base, a, peer, off) in enumerate(colors):
        mine = part.at[pl.ds(pl.multiple_of(off, 8), SMALL)]
        mine[...] = (mine[...] + r3[color, 2]) + (r3[color, 1] + r3[color, 3])

    load_q.wait()
    load_own.wait()

    def chunk(at):
        return qv.at[pl.ds(pl.multiple_of(at * 32, 32), 32)]

    sem_q = sems(4)
    source = (core == 1) & (x == y)
    receiver = (core == 1) & (x != y)

    @pl.when(jnp.logical_not(receiver))
    def _():
        qb[0] = qv[pl.ds(pl.multiple_of(x * 32, 32), 32), :]

    row_peers = (None, yp, yo, ym)
    for d in (1, 2, 3):

        @pl.when(source)
        def _():
            copy(chunk((y + d) % 4), qb.at[0], row_peers[d], sem_q + d, sem_q).start()

    def row_of(tile):
        late = tile // 9
        row = (1 - late) * (off_a + tile * 8) + late * (off_b + (tile - 9) * 8)
        return pl.multiple_of(row, 8)

    def tile_of(ref, tile):
        return ref.at[pl.ds(row_of(tile), 8)]

    my_held = held.at[core]
    sz, sz2 = sems(NZ), sems(NZ)
    for d in FAR_FIRST:
        dest = (z + d) % NZ
        push(tile_of(part, dest), zr.at[z], zs[d], sz + d, sz + z)
    for d in FAR_FIRST:
        dest = (z + d) % NZ

        @pl.when(dest < TILES - NZ)
        def _():
            copy(tile_of(part, dest + NZ), zr2.at[z], zs[d], sz2 + d, sz2 + z).start()

    zr[z] = part[pl.ds(row_of(z), 8), :]
    for d in FAR_FIRST:
        src = (z + NZ - d) % NZ
        copy(zr.at[src], zr.at[src], zs[d], sz + d, sz + src).wait_recv()
    total = zr[0]
    for n in range(1, NZ):
        total = total + zr[n]
    my_held[pl.ds(row_of(z), 8), :] = total

    @pl.when(z < TILES - NZ)
    def _():
        zr2[z] = part[pl.ds(row_of(z + NZ), 8), :]
        for d in FAR_FIRST:
            src = (z + NZ - d) % NZ
            copy(zr2.at[src], zr2.at[src], zs[d], sz2 + d, sz2 + src).wait_recv()
        total = zr2[0]
        for n in range(1, NZ):
            total = total + zr2[n]
        my_held[pl.ds(row_of(z + NZ), 8), :] = total

    gz, gz2 = sems(NZ), sems(NZ)
    mine = tile_of(my_held, z)
    for d in FAR_FIRST:
        push(mine, mine, zs[d], gz + d, gz + z)

    @pl.when(z < TILES - NZ)
    def _():
        mine = tile_of(my_held, z + NZ)
        for d in FAR_FIRST:
            copy(mine, mine, zs[d], gz2 + d, gz2 + z).start()

    for d in FAR_FIRST:
        src = (z + NZ - d) % NZ
        got = tile_of(my_held, src)
        copy(got, got, zs[d], gz + d, gz + src).wait_recv()
    for n in range(TILES - NZ):

        @pl.when(z != n)
        def _():
            got = tile_of(my_held, n + NZ)
            copy(got, got, zs[1], gz2 + 1, gz2 + n).wait_recv()

    class Gather:
        def __init__(self, whole, f, s, first, second):
            self.whole, self.f, self.s = whole, f, s
            self.first, self.second = first, second
            self.first_sem = sems(4)
            self.second_sem = [sems(4) for _ in range(4)]
            self.pair = sems(16)

        def chunk(self, n, m):
            return self.whole((self.f + n) % 4, (self.s + m) % 4)

        def wait(self, ref, sem):
            copy(ref, ref, other, sem, sem).wait_recv()

        def start(self):
            mine = self.chunk(0, 0)
            for n in (1, 3, 2):
                push(mine, mine, self.first[n - 1], self.first_sem + n)

        def landed(self, n):
            self.wait(self.chunk(n, 0), self.first_sem + 4 - n)

        def send(self, n):
            ref = self.chunk(n, 0)
            for m in (1, 3, 2):
                push(ref, ref, self.second[m - 1], self.second_sem[n] + m)
            self.hand(n, 0)

        def arrived(self, n, m):
            self.wait(self.chunk(n, m), self.second_sem[n] + 4 - m)
            self.hand(n, m)

        def paired(self, n, m):
            return self.chunk(n, m), self.pair + n * 4 + m

        def hand(self, n, m):
            ref, sem = self.paired(n, m)
            push(ref, ref, other, sem)

        def handed(self, n):
            for m in range(4):
                self.wait(*self.paired(n, m))

    def gather(both, ready):
        for g in both:
            g.start()
        for g in both:
            g.send(0)
        for n in (3, 1, 2):
            for g in both:
                g.landed(n)
                g.send(n)
        for n in (0, 3, 1, 2):
            for m in (3, 1, 2):
                for g in both:
                    g.arrived(n, m)
            ready(n)

    def held_rows(base):
        def whole(f, s):
            return my_held.at[pl.ds(pl.multiple_of(base + s * BIG + f * SMALL, 8), SMALL)]

        return whole

    sem_f = sems()

    @pl.when(receiver)
    def _():
        copy(qb.at[0], qb.at[0], yp, sem_q, sem_q).wait_recv()

    @pl.when(odd == 1)
    def _():
        copy(qb.at[0], qb.at[1], far, sem_f, sem_f).start()

    both = [
        Gather(held_rows(base_a), y, x, (yp, yo, ym), (xp, xo, xm)),
        Gather(held_rows(base_b), x, y, (xp, xo, xm), (yp, yo, ym)),
    ]
    gather(both, lambda n: None)
    colsum[...] = jnp.zeros_like(colsum)
    trace[...] = jnp.zeros_like(trace)
    row_id = lax.broadcasted_iota(jnp.int32, (128, 128), 0)
    col_id = lax.broadcasted_iota(jnp.int32, (128, 128), 1)

    def place(block, i, j):
        at = (slice(i * 128, (i + 1) * 128), slice(j * 128, (j + 1) * 128))
        first = block.astype(BF16)
        left = block - first.astype(F32)
        second = left.astype(BF16)
        g0[at] = first
        g1[at] = second
        if i == j:
            third = jnp.where(row_id == col_id, left - second.astype(F32), 0.0)
            rest[:, at[1]] = jnp.sum(third, axis=0, keepdims=True)
        colsum[:, at[1]] += jnp.sum(jnp.abs(block).reshape(16, 8, 128), axis=0)

    def place_owned(owner):
        for i in OWNED[owner]:
            for j in range(i, NB):
                slot = SLOTS[i, j][1]
                block = held[owner, slot * 128 : (slot + 1) * 128, :]
                place(block, i, j)
                if i == j:
                    diag = jnp.where(row_id == col_id, block, 0.0)
                    trace[...] += jnp.sum(diag.reshape(16, 8, 128), axis=0)
                else:
                    place(block.T, j, i)

    for which in (0, 1):

        @pl.when(core == which)
        def _():
            place_owned(which)

    for n in range(4):
        for g in both:
            g.handed(n)
    for which in (0, 1):

        @pl.when(core != which)
        def _():
            place_owned(which)

    total_rows = ROWS * lax.axis_size("grp") * lax.axis_size("dev")
    scale = 1.0 / total_rows
    trace_all = jnp.sum(jnp.sum(trace[...], axis=0, keepdims=True), axis=1, keepdims=True)
    damp = DAMPING * trace_all / (total_rows * K)
    sums = jnp.sum(colsum[...], axis=0, keepdims=True) * scale
    bound = jnp.max(sums, axis=1, keepdims=True) + damp
    step = 1.0 / bound

    @pl.when(odd == 1)
    def _():
        copy(qb.at[0], qb.at[1], far, sem_f, sem_f).wait_recv()

    ys[...] = step * qb[odd].astype(F32)

    def iterate(_, carry):
        for n, value in enumerate(split3(ys[...])):
            xs[n * 32 : (n + 1) * 32, :] = value
        for n in range(4):
            at = slice(n * 256, (n + 1) * 256)
            mid = jnp.dot(xs[0:64], g1[:, at], preferred_element_type=F32)
            top = jnp.dot(xs[...], g0[:, at], preferred_element_type=F32)
            state = ys[:, at]
            prod = top[0:32] + (top[32:64] + mid[0:32] + (top[64:96] + mid[32:64] + state * rest[:, at]))
            query = qb[odd, :, at].astype(F32)
            ys[:, at] = state + step * (query - (prod * scale + damp * state))
        return carry

    lax.fori_loop(0, ITERS, iterate, 0)

    first_at, second_at = (1 - core) * y + core * x, (1 - core) * x + core * y

    def along(step, first):
        dx = step * (core if first else 1 - core)
        dy = step * (1 - core if first else core)
        return where((x + dx) % 4, (y + dy) % 4, z, core)

    pa[core, first_at, second_at] = ys[...].astype(BF16)

    out_sem = sems(8)
    send_near.wait_recv()
    kept = []

    def scores(far, n):
        which = (1 - far) * core + far * (1 - core)
        block = ((second_at if far else first_at) + n) % 4
        slot = far * 4 + n
        found = nt_dot(tq[...], pa[which, block].reshape(128, K)).astype(BF16)
        ob[slot, 0] = found[0:ROWS]
        ob[slot, 1] = found[ROWS : 2 * ROWS]
        col = pl.multiple_of((block * 4 + near_half * 2 + which) * 128, 128)
        push(ob.at[slot, 1], out_hbm.at[:, pl.ds(col, 128)], neighbour, out_sem + slot)
        keep = pltpu.make_async_copy(
            ob.at[slot, 0], out_hbm.at[:, pl.ds(col, 128)], local_sem.at[3 + slot]
        )
        keep.start()
        kept.append(keep)

    prepared = Gather(
        lambda f, s: pa.at[core, f, s],
        first_at,
        second_at,
        [along(n, True) for n in (1, 2, 3)],
        [along(n, False) for n in (1, 2, 3)],
    )

    def handed(n):
        for m in range(4):
            ref = pa.at[1 - core, (second_at + n) % 4, (first_at + m) % 4]
            sem = prepared.pair + n * 4 + m
            copy(ref, ref, other, sem, sem).wait_recv()

    def ready(n):
        scores(0, n)
        if n in (3, 1):
            done = 0 if n == 3 else 3
            handed(done)
            scores(1, done)

    gather([prepared], ready)
    for n in (1, 2):
        handed(n)
        scores(1, n)
    for slot in range(8):
        far, n = slot // 4, slot % 4
        which = (1 - far) * core + far * (1 - core)
        block = ((second_at if far else first_at) + n) % 4
        col = pl.multiple_of((block * 4 + (1 - near_half) * 2 + which) * 128, 128)
        ref = out_hbm.at[:, pl.ds(col, 128)]
        copy(ob.at[slot, 1], ref, neighbour, out_sem + slot, out_sem + slot).wait_recv()

    for keep in kept:
        keep.wait()
    for made in started:
        made.wait_send()

    for d in (1, 2, 3):

        @pl.when(source)
        def _():
            copy(chunk((y + d) % 4), qb.at[0], row_peers[d], sem_q + d, sem_q).wait_send()

    @pl.when(odd == 1)
    def _():
        copy(qb.at[0], qb.at[1], far, sem_f, sem_f).wait_send()

    for d in FAR_FIRST:
        dest = (z + d) % NZ

        @pl.when(dest < TILES - NZ)
        def _():
            copy(tile_of(part, dest + NZ), zr2.at[z], zs[d], sz2 + d, sz2 + z).wait_send()

        @pl.when(z < TILES - NZ)
        def _():
            mine = tile_of(my_held, z + NZ)
            copy(mine, mine, zs[d], gz2 + d, gz2 + z).wait_send()


def body(train_grads, queries):
    nquery = queries.shape[0] * lax.axis_size("grp")
    return pl.pallas_call(
        kernel,
        out_shape=jax.ShapeDtypeStruct((ROWS, nquery), BF16),
        in_specs=[pl.BlockSpec(memory_space=pltpu.HBM)] * 2,
        out_specs=pl.BlockSpec(memory_space=pltpu.HBM),
        scratch_shapes=[
            pltpu.VMEM((2 * ROWS, K), BF16),
            pltpu.VMEM((2 * ROWS, K), BF16),
            pltpu.VMEM((ROWS, K), BF16),
            pltpu.VMEM((2, 32, K), BF16),
            pltpu.VMEM((HELD, 128), F32),
            pltpu.VMEM((2, HELD, 128), F32),
            pltpu.VMEM((2, 2, BIG // 2, 128), F32),
            pltpu.VMEM((2, 2, BIG, 128), F32),
            pltpu.VMEM((2, 4, SMALL, 128), F32),
            pltpu.VMEM((NZ, 8, 128), F32),
            pltpu.VMEM((NZ, 8, 128), F32),
            pltpu.VMEM((K, K), BF16),
            pltpu.VMEM((K, K), BF16),
            pltpu.VMEM((1, K), F32),
            pltpu.VMEM((8, K), F32),
            pltpu.VMEM((8, 128), F32),
            pltpu.VMEM((96, K), BF16),
            pltpu.VMEM((32, K), F32),
            pltpu.VMEM((2, 4, 4, 32, K), BF16),
            pltpu.VMEM((8, 2, ROWS, 128), BF16),
            pltpu.SemaphoreType.DMA((NSEM,)),
            pltpu.SemaphoreType.DMA((NSEM,)),
            pltpu.SemaphoreType.DMA((11,)),
        ],
        compiler_params=pltpu.CompilerParams(
            collective_id=0, has_side_effects=True, vmem_limit_bytes=63 * 1024 * 1024
        ),
    )(train_grads, queries)


def solution(mesh):
    return jax.shard_map(
        body,
        mesh=mesh,
        in_specs=(P(("grp", "dev"), None), P("grp", None)),
        out_specs=P(("grp", "dev"), None),
        check_vma=False,
    )
```

```python
import jax
import jax.numpy as jnp
from jax import lax
from jax.experimental import pallas as pl
from jax.experimental.pallas import tpu as pltpu
from jax.sharding import PartitionSpec as P

MESH = pl.DeviceIdType.MESH
F32, BF16 = jnp.float32, jnp.bfloat16
ITERS = 8
DAMPING = 0.1
K = 1024
ROWS = 128
NB = K // 128
NX = NY = 4
NZ = 16
OWNED = ((0, 3, 4, 7), (1, 2, 5, 6))
SLOTS = {}
for _core, _rows in enumerate(OWNED):
    for _slot, _ij in enumerate((i, j) for i in _rows for j in range(i, NB)):
        SLOTS[_ij] = (_core, _slot)
NSLOT = 18
HELD = NSLOT * 128
HALF = HELD // 2
BIG = HALF // 4
SMALL = BIG // 4
TILES = 2 * SMALL // 8
CUT_BIG = (0, 144, 288)
NSEM = 320
FAR_FIRST = sorted(range(1, NZ), key=lambda d: -min(d, NZ - d))


def split3(value):
    first = value.astype(BF16)
    rest = value - first.astype(F32)
    second = rest.astype(BF16)
    third = (rest - second.astype(F32)).astype(BF16)
    return first, second, third


def nt_dot(left, right):
    return lax.dot_general(left, right, (((1,), (1,)), ((), ())), preferred_element_type=F32)


def kernel(
    t_hbm, q_hbm, out_hbm,
    tt, tq, qv, qb, part, held, r1, r2, r3, zr, zr2, g0, g1, rest, colsum, trace, xs, ys, pa, ob,
    send_sem, recv_sem, local_sem,
):
    grp, dev = lax.axis_index("grp"), lax.axis_index("dev")
    y, zh, core = grp // 4, (grp // 2) % 2, grp % 2
    x, z = dev % 4, zh * 8 + dev // 4

    def where(px, py, pz, pc):
        return (py * 4 + (pz // 8) * 2 + pc, (pz % 8) * 4 + px)

    other = where(x, y, z, 1 - core)
    xp, xm = where((x + 1) % 4, y, z, core), where((x + 3) % 4, y, z, core)
    yp, ym = where(x, (y + 1) % 4, z, core), where(x, (y + 3) % 4, z, core)
    xo, yo = where((x + 2) % 4, y, z, core), where(x, (y + 2) % 4, z, core)
    zs = [where(x, y, (z + d) % NZ, core) for d in range(NZ)]
    odd = z % 2
    neighbour = where(x, y, z + 1 - 2 * odd, core)
    near_half = (zh + odd) % 2
    far = where(x, y, (z + 8) % NZ, core)

    started = []
    used = [0]

    def sems(n=1):
        base = used[0]
        used[0] += n
        assert used[0] <= NSEM
        return base

    def copy(src, dst, device, send, recv):
        return pltpu.make_async_remote_copy(
            src_ref=src, dst_ref=dst, send_sem=send_sem.at[send], recv_sem=recv_sem.at[recv],
            device_id=device, device_id_type=MESH,
        )

    def push(src, dst, device, send, recv=None):
        made = copy(src, dst, device, send, send if recv is None else recv)
        made.start()
        started.append(made)
        return made

    barrier = pltpu.get_barrier_semaphore()
    peers = [other, xp, xm, xo, yp, ym, yo] + zs[1:]
    for peer in peers:
        pl.semaphore_signal(barrier, inc=1, device_id=peer, device_id_type=MESH)
    mine_t = tt.at[pl.ds(pl.multiple_of(core * ROWS, ROWS), ROWS)]
    load_t = pltpu.make_async_copy(t_hbm, mine_t, local_sem.at[0])
    load_q = pltpu.make_async_copy(q_hbm, qv, local_sem.at[1])
    load_own = pltpu.make_async_copy(t_hbm, tq.at[pl.ds(0, ROWS)], local_sem.at[2])
    load_t.start()
    load_q.start()
    load_own.start()
    load_t.wait()
    pl.semaphore_wait(barrier, len(peers))

    send_t = push(mine_t, mine_t, other, sems())
    send_near = push(mine_t, tq.at[pl.ds(ROWS, ROWS)], neighbour, sems())
    send_t.wait_recv()

    def gram_rows(rows, cols):
        left = tt[:, rows * 128 : (rows + 1) * 128]
        right = tt[:, cols[0] * 128 : (cols[-1] + 1) * 128]
        return lax.dot_general(left, right, (((0,), (0,)), ((), ())), preferred_element_type=F32)

    for which in (0, 1):

        @pl.when(core == which)
        def _():
            for i in OWNED[which]:
                cols = list(range(i, NB))
                block = gram_rows(i, cols)
                for at, j in enumerate(cols):
                    slot = SLOTS[i, j][1]
                    part[slot * 128 : (slot + 1) * 128, :] = block[:, at * 128 : (at + 1) * 128]

    class Reduce:
        def __init__(self, base, cut, at, plus, minus, recv1, recv2, color):
            self.base, self.cut, self.at, self.plus, self.minus = base, cut, at, plus, minus
            self.r1, self.r2 = recv1, recv2
            self.color, self.sem = color, sems(6)
            self.moves = {}

        def piece(self, which, half):
            lo, hi = self.cut[half], self.cut[half + 1]
            row = self.base + which * self.cut[2] + lo
            return part.at[pl.ds(pl.multiple_of(row, 8), hi - lo)]

        def first(self, side):
            half = side
            return self.r1.at[self.color, side, pl.ds(0, self.cut[half + 1] - self.cut[half])]

        def second(self, side, half):
            lo, hi = self.cut[half], self.cut[half + 1]
            return self.r2.at[self.color, side, pl.ds(lo, hi - lo)]

        def start(self):
            a, s = self.at, self.sem
            self.moves[0] = push(self.piece((a + 2) % 4, 0), self.first(0), self.plus, s)
            self.moves[1] = push(self.piece((a + 2) % 4, 1), self.first(1), self.minus, s + 1)
            self.moves[2] = push(self.piece((a + 1) % 4, 1), self.second(0, 1), self.plus, s + 2)
            self.moves[3] = push(self.piece((a + 3) % 4, 0), self.second(1, 0), self.minus, s + 3)

        def middle(self):
            a, s = self.at, self.sem
            self.moves[0].wait_recv()
            mine = self.piece((a + 1) % 4, 0)
            mine[...] = mine[...] + self.first(0)[...]
            self.moves[1].wait_recv()
            mine1 = self.piece((a + 3) % 4, 1)
            mine1[...] = mine1[...] + self.first(1)[...]
            self.moves[4] = push(mine, self.second(0, 0), self.plus, s + 4)
            self.moves[5] = push(mine1, self.second(1, 1), self.minus, s + 5)

        def finish(self):
            for n in (2, 3, 4, 5):
                self.moves[n].wait_recv()
            row = self.base + self.at * self.cut[2]
            mine = part.at[pl.ds(pl.multiple_of(row, 8), self.cut[2])]
            total = mine[...] + self.r2[self.color, 0] + self.r2[self.color, 1]
            return mine, total

    base_a, base_b = 0, HALF
    red = [
        Reduce(base_a, CUT_BIG, x, xp, xm, r1, r2, 0),
        Reduce(base_b, CUT_BIG, y, yp, ym, r1, r2, 1),
    ]
    for r in red:
        r.start()
    for r in red:
        r.middle()
    for r in red:
        mine, total = r.finish()
        mine[...] = total
    off_a = base_a + x * BIG + y * SMALL
    off_b = base_b + y * BIG + x * SMALL
    colors = (
        (base_a + x * BIG, y, (None, yp, yo, ym), off_a),
        (base_b + y * BIG, x, (None, xp, xo, xm), off_b),
    )
    cross = [sems(4), sems(4)]
    moves = []
    for n in (2, 1, 3):
        for color, (base, a, peer, _) in enumerate(colors):
            row = pl.multiple_of(base + ((a + n) % 4) * SMALL, 8)
            moves.append(push(part.at[pl.ds(row, SMALL)], r3.at[color, n], peer[n], cross[color] + n))
    for made in moves:
        made.wait_recv()
    for color, (base, a, peer, off) in enumerate(colors):
        mine = part.at[pl.ds(pl.multiple_of(off, 8), SMALL)]
        mine[...] = (mine[...] + r3[color, 2]) + (r3[color, 1] + r3[color, 3])

    load_q.wait()
    load_own.wait()

    def chunk(at):
        return qv.at[pl.ds(pl.multiple_of(at * 32, 32), 32)]

    sem_q = sems(4)
    source = (core == 1) & (x == y)
    receiver = (core == 1) & (x != y)

    @pl.when(jnp.logical_not(receiver))
    def _():
        qb[0] = qv[pl.ds(pl.multiple_of(x * 32, 32), 32), :]

    row_peers = (None, yp, yo, ym)
    for d in (1, 2, 3):

        @pl.when(source)
        def _():
            copy(chunk((y + d) % 4), qb.at[0], row_peers[d], sem_q + d, sem_q).start()

    def row_of(tile):
        late = tile // 9
        row = (1 - late) * (off_a + tile * 8) + late * (off_b + (tile - 9) * 8)
        return pl.multiple_of(row, 8)

    def tile_of(ref, tile):
        return ref.at[pl.ds(row_of(tile), 8)]

    my_held = held.at[core]
    sz, sz2 = sems(NZ), sems(NZ)
    for d in FAR_FIRST:
        dest = (z + d) % NZ
        push(tile_of(part, dest), zr.at[z], zs[d], sz + d, sz + z)
    for d in FAR_FIRST:
        dest = (z + d) % NZ

        @pl.when(dest < TILES - NZ)
        def _():
            copy(tile_of(part, dest + NZ), zr2.at[z], zs[d], sz2 + d, sz2 + z).start()

    zr[z] = part[pl.ds(row_of(z), 8), :]
    for d in FAR_FIRST:
        src = (z + NZ - d) % NZ
        copy(zr.at[src], zr.at[src], zs[d], sz + d, sz + src).wait_recv()
    total = zr[0]
    for n in range(1, NZ):
        total = total + zr[n]
    my_held[pl.ds(row_of(z), 8), :] = total

    @pl.when(z < TILES - NZ)
    def _():
        zr2[z] = part[pl.ds(row_of(z + NZ), 8), :]
        for d in FAR_FIRST:
            src = (z + NZ - d) % NZ
            copy(zr2.at[src], zr2.at[src], zs[d], sz2 + d, sz2 + src).wait_recv()
        total = zr2[0]
        for n in range(1, NZ):
            total = total + zr2[n]
        my_held[pl.ds(row_of(z + NZ), 8), :] = total

    gz, gz2 = sems(NZ), sems(NZ)
    mine = tile_of(my_held, z)
    for d in FAR_FIRST:
        push(mine, mine, zs[d], gz + d, gz + z)

    @pl.when(z < TILES - NZ)
    def _():
        mine = tile_of(my_held, z + NZ)
        for d in FAR_FIRST:
            copy(mine, mine, zs[d], gz2 + d, gz2 + z).start()

    for d in FAR_FIRST:
        src = (z + NZ - d) % NZ
        got = tile_of(my_held, src)
        copy(got, got, zs[d], gz + d, gz + src).wait_recv()
    for n in range(TILES - NZ):

        @pl.when(z != n)
        def _():
            got = tile_of(my_held, n + NZ)
            copy(got, got, zs[1], gz2 + 1, gz2 + n).wait_recv()

    class Gather:
        def __init__(self, whole, f, s, first, second):
            self.whole, self.f, self.s = whole, f, s
            self.first, self.second = first, second
            self.first_sem = sems(4)
            self.second_sem = [sems(4) for _ in range(4)]
            self.pair = sems(16)

        def chunk(self, n, m):
            return self.whole((self.f + n) % 4, (self.s + m) % 4)

        def wait(self, ref, sem):
            copy(ref, ref, other, sem, sem).wait_recv()

        def start(self):
            mine = self.chunk(0, 0)
            for n in (1, 3, 2):
                push(mine, mine, self.first[n - 1], self.first_sem + n)

        def landed(self, n):
            self.wait(self.chunk(n, 0), self.first_sem + 4 - n)

        def send(self, n):
            ref = self.chunk(n, 0)
            for m in (1, 3, 2):
                push(ref, ref, self.second[m - 1], self.second_sem[n] + m)
            self.hand(n, 0)

        def arrived(self, n, m):
            self.wait(self.chunk(n, m), self.second_sem[n] + 4 - m)
            self.hand(n, m)

        def paired(self, n, m):
            return self.chunk(n, m), self.pair + n * 4 + m

        def hand(self, n, m):
            ref, sem = self.paired(n, m)
            push(ref, ref, other, sem)

        def handed(self, n):
            for m in range(4):
                self.wait(*self.paired(n, m))

    def gather(both, ready):
        for g in both:
            g.start()
        for g in both:
            g.send(0)
        for n in (3, 1, 2):
            for g in both:
                g.landed(n)
                g.send(n)
        for n, behind in ((0, None), (3, 0), (1, 3), (2, 1)):
            for m in (3, 1):
                for g in both:
                    g.arrived(n, m)
            if behind is not None:
                ready(behind)
            for g in both:
                g.arrived(n, 2)
        ready(2)

    def held_rows(base):
        def whole(f, s):
            return my_held.at[pl.ds(pl.multiple_of(base + s * BIG + f * SMALL, 8), SMALL)]

        return whole

    sem_f = sems()

    @pl.when(receiver)
    def _():
        copy(qb.at[0], qb.at[0], yp, sem_q, sem_q).wait_recv()

    @pl.when(odd == 1)
    def _():
        copy(qb.at[0], qb.at[1], far, sem_f, sem_f).start()

    both = [
        Gather(held_rows(base_a), y, x, (yp, yo, ym), (xp, xo, xm)),
        Gather(held_rows(base_b), x, y, (xp, xo, xm), (yp, yo, ym)),
    ]
    gather(both, lambda n: None)
    colsum[...] = jnp.zeros_like(colsum)
    trace[...] = jnp.zeros_like(trace)
    row_id = lax.broadcasted_iota(jnp.int32, (128, 128), 0)
    col_id = lax.broadcasted_iota(jnp.int32, (128, 128), 1)

    def place(block, i, j):
        at = (slice(i * 128, (i + 1) * 128), slice(j * 128, (j + 1) * 128))
        first = block.astype(BF16)
        left = block - first.astype(F32)
        second = left.astype(BF16)
        g0[at] = first
        g1[at] = second
        if i == j:
            third = jnp.where(row_id == col_id, left - second.astype(F32), 0.0)
            rest[:, at[1]] = jnp.sum(third, axis=0, keepdims=True)
        colsum[:, at[1]] += jnp.sum(jnp.abs(block).reshape(16, 8, 128), axis=0)

    def place_owned(owner):
        for i in OWNED[owner]:
            for j in range(i, NB):
                slot = SLOTS[i, j][1]
                block = held[owner, slot * 128 : (slot + 1) * 128, :]
                place(block, i, j)
                if i == j:
                    diag = jnp.where(row_id == col_id, block, 0.0)
                    trace[...] += jnp.sum(diag.reshape(16, 8, 128), axis=0)
                else:
                    place(block.T, j, i)

    for which in (0, 1):

        @pl.when(core == which)
        def _():
            place_owned(which)

    for n in range(4):
        for g in both:
            g.handed(n)
    for which in (0, 1):

        @pl.when(core != which)
        def _():
            place_owned(which)

    total_rows = ROWS * lax.axis_size("grp") * lax.axis_size("dev")
    scale = 1.0 / total_rows
    trace_all = jnp.sum(jnp.sum(trace[...], axis=0, keepdims=True), axis=1, keepdims=True)
    damp = DAMPING * trace_all / (total_rows * K)
    sums = jnp.sum(colsum[...], axis=0, keepdims=True) * scale
    bound = jnp.max(sums, axis=1, keepdims=True) + damp
    step = 1.0 / bound

    @pl.when(odd == 1)
    def _():
        copy(qb.at[0], qb.at[1], far, sem_f, sem_f).wait_recv()

    ys[...] = step * qb[odd].astype(F32)

    def iterate(_, carry):
        for n, value in enumerate(split3(ys[...])):
            xs[n * 32 : (n + 1) * 32, :] = value
        for n in range(4):
            at = slice(n * 256, (n + 1) * 256)
            mid = jnp.dot(xs[0:64], g1[:, at], preferred_element_type=F32)
            top = jnp.dot(xs[...], g0[:, at], preferred_element_type=F32)
            state = ys[:, at]
            prod = top[0:32] + (top[32:64] + mid[0:32] + (top[64:96] + mid[32:64] + state * rest[:, at]))
            query = qb[odd, :, at].astype(F32)
            ys[:, at] = state + step * (query - (prod * scale + damp * state))
        return carry

    lax.fori_loop(0, ITERS, iterate, 0)

    first_at, second_at = (1 - core) * y + core * x, (1 - core) * x + core * y

    def along(step, first):
        dx = step * (core if first else 1 - core)
        dy = step * (1 - core if first else core)
        return where((x + dx) % 4, (y + dy) % 4, z, core)

    pa[core, first_at, second_at] = ys[...].astype(BF16)

    out_sem = sems(8)
    send_near.wait_recv()
    kept = []

    def scores(far, n):
        which = (1 - far) * core + far * (1 - core)
        block = ((second_at if far else first_at) + n) % 4
        slot = far * 4 + n
        found = nt_dot(tq[...], pa[which, block].reshape(128, K)).astype(BF16)
        ob[slot, 0] = found[0:ROWS]
        ob[slot, 1] = found[ROWS : 2 * ROWS]
        col = pl.multiple_of((block * 4 + near_half * 2 + which) * 128, 128)
        push(ob.at[slot, 1], out_hbm.at[:, pl.ds(col, 128)], neighbour, out_sem + slot)
        keep = pltpu.make_async_copy(
            ob.at[slot, 0], out_hbm.at[:, pl.ds(col, 128)], local_sem.at[3 + slot]
        )
        keep.start()
        kept.append(keep)

    prepared = Gather(
        lambda f, s: pa.at[core, f, s],
        first_at,
        second_at,
        [along(n, True) for n in (1, 2, 3)],
        [along(n, False) for n in (1, 2, 3)],
    )

    def handed(n):
        for m in range(4):
            ref = pa.at[1 - core, (second_at + n) % 4, (first_at + m) % 4]
            sem = prepared.pair + n * 4 + m
            copy(ref, ref, other, sem, sem).wait_recv()

    def ready(n):
        scores(0, n)
        if n in (3, 1):
            done = 0 if n == 3 else 3
            handed(done)
            scores(1, done)

    gather([prepared], ready)
    for n in (1, 2):
        handed(n)
        scores(1, n)
    for slot in range(8):
        far, n = slot // 4, slot % 4
        which = (1 - far) * core + far * (1 - core)
        block = ((second_at if far else first_at) + n) % 4
        col = pl.multiple_of((block * 4 + (1 - near_half) * 2 + which) * 128, 128)
        ref = out_hbm.at[:, pl.ds(col, 128)]
        copy(ob.at[slot, 1], ref, neighbour, out_sem + slot, out_sem + slot).wait_recv()

    for keep in kept:
        keep.wait()
    for made in started:
        made.wait_send()

    for d in (1, 2, 3):

        @pl.when(source)
        def _():
            copy(chunk((y + d) % 4), qb.at[0], row_peers[d], sem_q + d, sem_q).wait_send()

    @pl.when(odd == 1)
    def _():
        copy(qb.at[0], qb.at[1], far, sem_f, sem_f).wait_send()

    for d in FAR_FIRST:
        dest = (z + d) % NZ

        @pl.when(dest < TILES - NZ)
        def _():
            copy(tile_of(part, dest + NZ), zr2.at[z], zs[d], sz2 + d, sz2 + z).wait_send()

        @pl.when(z < TILES - NZ)
        def _():
            mine = tile_of(my_held, z + NZ)
            copy(mine, mine, zs[d], gz2 + d, gz2 + z).wait_send()


def body(train_grads, queries):
    nquery = queries.shape[0] * lax.axis_size("grp")
    return pl.pallas_call(
        kernel,
        out_shape=jax.ShapeDtypeStruct((ROWS, nquery), BF16),
        in_specs=[pl.BlockSpec(memory_space=pltpu.HBM)] * 2,
        out_specs=pl.BlockSpec(memory_space=pltpu.HBM),
        scratch_shapes=[
            pltpu.VMEM((2 * ROWS, K), BF16),
            pltpu.VMEM((2 * ROWS, K), BF16),
            pltpu.VMEM((ROWS, K), BF16),
            pltpu.VMEM((2, 32, K), BF16),
            pltpu.VMEM((HELD, 128), F32),
            pltpu.VMEM((2, HELD, 128), F32),
            pltpu.VMEM((2, 2, BIG // 2, 128), F32),
            pltpu.VMEM((2, 2, BIG, 128), F32),
            pltpu.VMEM((2, 4, SMALL, 128), F32),
            pltpu.VMEM((NZ, 8, 128), F32),
            pltpu.VMEM((NZ, 8, 128), F32),
            pltpu.VMEM((K, K), BF16),
            pltpu.VMEM((K, K), BF16),
            pltpu.VMEM((1, K), F32),
            pltpu.VMEM((8, K), F32),
            pltpu.VMEM((8, 128), F32),
            pltpu.VMEM((96, K), BF16),
            pltpu.VMEM((32, K), F32),
            pltpu.VMEM((2, 4, 4, 32, K), BF16),
            pltpu.VMEM((8, 2, ROWS, 128), BF16),
            pltpu.SemaphoreType.DMA((NSEM,)),
            pltpu.SemaphoreType.DMA((NSEM,)),
            pltpu.SemaphoreType.DMA((11,)),
        ],
        compiler_params=pltpu.CompilerParams(
            collective_id=0, has_side_effects=True, vmem_limit_bytes=63 * 1024 * 1024
        ),
    )(train_grads, queries)


def solution(mesh):
    return jax.shard_map(
        body,
        mesh=mesh,
        in_specs=(P(("grp", "dev"), None), P("grp", None)),
        out_specs=P(("grp", "dev"), None),
        check_vma=False,
    )
```
